512 devices in a mesh: row: 32 (over z, x), col: 16 (over y, core).
Axes of the slice: x: 4, y: 8, z: 8, core: 2. Of those that a mesh axis runs over, the one named last changes fastest.
Arguments:
- field: bfloat16 [1, 64, 2048, 2048], P(None, None, 'row', 'col'), may hold values from -6 to 6
- x_weight: float32 [2, 2, 12, 64, 64], replicated, may hold values from -2 to 2
- y_weight: float32 [2, 2, 12, 64, 64], replicated, may hold values from -2 to 2
- up_weight: bfloat16 [2, 256, 64], replicated, may hold values from -0.75 to 0.75
- up_bias: float32 [2, 256], replicated, may hold values from -3 to 3
- down_weight: bfloat16 [2, 64, 256], replicated, may hold values from -0.375 to 0.375
Outputs:
- result: bfloat16 [1, 64, 2048, 2048], P(None, None, 'row', 'col')
The draws below stay inside these ranges and needn't reach their ends.
All inputs are finite; a program needn't handle non-finite values.
Results may differ from the reference program's by a relative error of at most 0.025.
Values may be sent and summed in bfloat16 or wider, within the bound.
No kernel may reach another device: no remote copies, remote signals or barrier semaphores. Data moves between devices by JAX's collectives and lax.ppermute only.
A program may use at most 64 MiB of HBM per device.

```python
import math
import jax
import jax.numpy as jnp
from jax import lax

C = 64
H = 256
MODES = 12
LAYERS = 2
Z = 1
NX = 2048
NY = 2048


def steps_of(own_key, dims, split, smallest, largest):
    loudness = 1.0
    for axis_at, shards_of in split:
        heights = jax.random.uniform(jax.random.fold_in(jax.random.fold_in(own_key, 6), axis_at), (shards_of,), jnp.float32, smallest / len(split), largest / len(split))
        loudness = loudness * jnp.repeat(jnp.exp(heights), dims[axis_at] // shards_of).reshape((-1,) + (1,) * (len(dims) - 1 - axis_at))
    return loudness


def normal_values(stream_key, extent, deviation, bound, split=(), kind=jnp.bfloat16):
    result = jax.random.normal(stream_key, extent, jnp.float32) * deviation
    if len(split) > 0:
        result = steps_of(stream_key, extent, split, -0.22, 0.18) * result
    return jnp.clip(result, min=-bound, max=bound).astype(kind)


def setup_inputs(seed: int = 0) -> dict:
    key_list = jax.random.split(jax.random.key(seed), 7)
    field = normal_values(key_list[0], (Z, C, NX, NY), 1.0, 6.0, ((2, 32), (3, 16)))
    x_weight = normal_values(key_list[1], (LAYERS, 2, MODES, C, C), 0.35, 2.0, (), jnp.float32)
    y_weight = normal_values(key_list[2], (LAYERS, 2, MODES, C, C), 0.35, 2.0, (), jnp.float32)
    up_weight = normal_values(key_list[3], (LAYERS, H, C), C ** -0.5, 0.75)
    up_bias = normal_values(key_list[4], (LAYERS, H), 0.5, 3.0, (), jnp.float32)
    down_weight = normal_values(key_list[5], (LAYERS, C, H), H ** -0.5, 0.375)
    return {"field": field, "x_weight": x_weight, "y_weight": y_weight, "up_weight": up_weight, "up_bias": up_bias, "down_weight": down_weight}


def tables(total, count):
    pos = jnp.arange(count, dtype=jnp.int32)
    kays = jnp.arange(MODES, dtype=jnp.int32)
    phase = (kays[:, None] * pos[None, :]) % total
    angle = phase.astype(jnp.float32) * (2.0 * math.pi / total)
    cosine = jnp.cos(angle)
    sine = jnp.sin(angle)
    forward = jnp.concatenate([cosine, -sine], axis=0).astype(jnp.bfloat16)
    factor = (jnp.where(kays == 0, 1.0, 2.0) / total).astype(jnp.float32)[:, None]
    inverse = jnp.concatenate([cosine * factor, -sine * factor], axis=0).astype(jnp.bfloat16)
    return forward, inverse


def mix_modes(modes, weight):
    first = modes[:, :MODES]
    second = modes[:, MODES:]
    hi = lax.Precision.HIGHEST
    real_part = jnp.einsum("kco,zkcr->zkor", weight[0], first, precision=hi) - jnp.einsum("kco,zkcr->zkor", weight[1], second, precision=hi)
    imag_part = jnp.einsum("kco,zkcr->zkor", weight[1], first, precision=hi) + jnp.einsum("kco,zkcr->zkor", weight[0], second, precision=hi)
    return jnp.concatenate([real_part, imag_part], axis=1).astype(jnp.bfloat16)


def feed_block(block, w_up, b_up, w_down):
    hidden = jnp.einsum("hc,zcxy->zhxy", w_up.astype(jnp.float32), block.astype(jnp.float32))
    hidden = jax.nn.gelu(hidden + b_up[None, :, None, None], approximate=False).astype(jnp.bfloat16)
    back = jnp.einsum("ch,zhxy->zcxy", w_down.astype(jnp.float32), hidden.astype(jnp.float32))
    return (block.astype(jnp.float32) + back).astype(jnp.bfloat16)


def reference(field, x_weight, y_weight, up_weight, up_bias, down_weight):
    fwd_x, inv_x = tables(NX, NX)
    fwd_y, inv_y = tables(NY, NY)
    block = 64
    state = field
    for layer in range(LAYERS):
        wide = state.astype(jnp.float32)
        xmodes = jnp.einsum("mx,zcxy->zmcy", fwd_x.astype(jnp.float32), wide)
        xmixed = mix_modes(xmodes, x_weight[layer])
        back_x = jnp.einsum("mx,zmoy->zoxy", inv_x.astype(jnp.float32), xmixed.astype(jnp.float32))
        ymodes = jnp.einsum("my,zcxy->zmcx", fwd_y.astype(jnp.float32), wide)
        ymixed = mix_modes(ymodes, y_weight[layer])
        back_y = jnp.einsum("my,zmox->zoxy", inv_y.astype(jnp.float32), ymixed.astype(jnp.float32))
        gfield = (wide + back_x + back_y).astype(jnp.bfloat16)
        pieces = gfield.reshape(Z, C, NX // block, block, NY).transpose(2, 0, 1, 3, 4)
        w_up = up_weight[layer]
        b_up = up_bias[layer]
        w_down = down_weight[layer]
        done = lax.map(lambda piece: feed_block(piece, w_up, b_up, w_down), pieces)
        state = done.transpose(1, 2, 0, 3, 4).reshape(Z, C, NX, NY)
    return state
```

```python
import functools
import math

import jax
import jax.numpy as jnp
from jax import lax
from jax.experimental import pallas as pl
from jax.experimental.pallas import tpu as pltpu
from jax.sharding import PartitionSpec as P

MODES = 12
ROWS = 2 * MODES
LAYERS = 2
ROOT_HALF = math.sqrt(0.5)
TN = (((0,), (0,)), ((), ()))
NT = (((1,), (1,)), ((), ()))
NN = (((1,), (0,)), ((), ()))


def dot(a, b, dims=NN):
    return lax.dot_general(a, b, dims, preferred_element_type=jnp.float32)


def table_pair(total, start, count):
    pos = start + jnp.arange(count, dtype=jnp.int32)
    kays = jnp.arange(MODES, dtype=jnp.int32)
    phase = kays[:, None] * pos[None, :] % total
    angle = phase.astype(jnp.float32) * (2.0 * math.pi / total)
    cosine = jnp.cos(angle)
    sine = jnp.sin(angle)
    forward = jnp.concatenate([cosine, -sine], axis=0).astype(jnp.bfloat16)
    factor = (jnp.where(kays == 0, 1.0, 2.0) / total).astype(jnp.float32)[:, None]
    inverse = jnp.concatenate([cosine * factor, -sine * factor], axis=0).astype(jnp.bfloat16)
    return forward, inverse


def mixing_matrices(weight):
    w0 = jnp.swapaxes(weight[0], 1, 2)
    w1 = jnp.swapaxes(weight[1], 1, 2)
    top = jnp.concatenate([w0, -w1], axis=2)
    bottom = jnp.concatenate([w1, w0], axis=2)
    return jnp.concatenate([top, bottom], axis=1).astype(jnp.bfloat16)


def strided(ref, start, size, stride, value):
    ref[pl.ds(start, size, stride=stride), :] = value


def forward_parts(state, fbx, fwd_y, mix_x, mix_y, out_x, out_y, qx, qy, rx, ry):
    chans, nx = state.chans, state.nx
    group = fbx.shape[1] // nx
    half = chans // 2
    sx, sy = qx.shape[0] // ROWS, qy.shape[0] // ROWS
    table = fbx[...]
    for c0 in range(0, chans, group):
        part = dot(table, jnp.concatenate([state(c0 + i) for i in range(group)], axis=0))
        for i in range(group):
            strided(qx, c0 + i, ROWS, sx, part[i * ROWS : (i + 1) * ROWS])
    table = fwd_y[...]
    for j in range(0, half, 2):
        both = jnp.concatenate(
            [state(j), state(j + half), state(j + 1), state(j + 1 + half)], axis=0
        )
        part = dot(table, both, NT)
        strided(qy, j, ROWS, sy, part[:, : 2 * nx])
        strided(qy, j + 1, ROWS, sy, part[:, 2 * nx :])
    for k in range(MODES):
        re = qx[k * sx : k * sx + chans]
        im = qx[(MODES + k) * sx : (MODES + k) * sx + chans]
        mixed = dot(mix_x[k], jnp.concatenate([re, im], axis=0).astype(jnp.bfloat16))
        strided(rx, k, chans, ROWS, mixed[:chans])
        strided(rx, MODES + k, chans, ROWS, mixed[chans:])
    for k in range(MODES):
        re = qy[k * sy : k * sy + half]
        im = qy[(MODES + k) * sy : (MODES + k) * sy + half]
        stack = jnp.concatenate([re[:, :nx], re[:, nx:], im[:, :nx], im[:, nx:]], axis=0)
        mixed = dot(mix_y[k], stack.astype(jnp.bfloat16))
        re = jnp.concatenate([mixed[:half], mixed[half:chans]], axis=1)
        im = jnp.concatenate([mixed[chans : chans + half], mixed[chans + half :]], axis=1)
        strided(ry, k, half, ROWS, re)
        strided(ry, MODES + k, half, ROWS, im)
    out_x[...] = rx[...].astype(jnp.bfloat16)
    out_y[...] = ry[...].astype(jnp.bfloat16)


class Planes:
    def __init__(self, ref):
        self.ref = ref
        self.chans, self.nx, _ = ref.shape

    def __call__(self, c):
        return self.ref[c]


def first_kernel(field, fbx, fwd_y, mix_x, mix_y, out_x, out_y, qx, qy, rx, ry):
    forward_parts(Planes(field), fbx, fwd_y, mix_x, mix_y, out_x, out_y, qx, qy, rx, ry)


def apply_layer(field, got_x, got_y, inv_xt, inv_y, up, bias, down, result, tmp):
    chans, nx, ny = field.shape
    half = chans // 2
    step = tmp.shape[0] // chans
    gx = inv_xt[...]
    gy = inv_y[...]
    for j in range(half):
        from_y = dot(got_y[j], gy, TN)
        for h in range(2):
            c = j + h * half
            back = dot(gx, got_x[c]) + from_y[h * nx : (h + 1) * nx]
            total = (field[c].astype(jnp.float32) + back).astype(jnp.bfloat16)
            tmp[c * step : c * step + nx] = total.astype(jnp.float32)
    group = 4

    def feed(i, carry):
        x0 = i * group
        blocks = [tmp[pl.ds(x0 + a, chans, stride=step), :] for a in range(group)]
        wide = jnp.concatenate(blocks, axis=1)
        hidden = dot(up[...], wide.astype(jnp.bfloat16)) + bias[...]
        hidden = hidden + hidden * lax.erf(hidden * ROOT_HALF)
        back = dot(down[...], hidden.astype(jnp.bfloat16))
        new = (wide + back).astype(jnp.bfloat16).astype(jnp.float32)
        for a in range(group):
            tmp[pl.ds(x0 + a, chans, stride=step), :] = new[:, a * ny : (a + 1) * ny]
        return carry

    lax.fori_loop(0, nx // group, feed, 0)
    for c in range(chans):
        result[c] = tmp[c * step : c * step + nx].astype(jnp.bfloat16)


def middle_kernel(
    field, got_x, got_y, inv_xt, inv_y, up, bias, down, fbx, fwd_y, mix_x, mix_y,
    result, out_x, out_y, tmp, qx, qy, rx, ry,
):
    apply_layer(field, got_x, got_y, inv_xt, inv_y, up, bias, down, result, tmp)
    forward_parts(Planes(result), fbx, fwd_y, mix_x, mix_y, out_x, out_y, qx, qy, rx, ry)


def last_kernel(field, got_x, got_y, inv_xt, inv_y, up, bias, down, result, tmp):
    apply_layer(field, got_x, got_y, inv_xt, inv_y, up, bias, down, result, tmp)


def call(kernel, outs, scratch, args, flops):
    vmem = pl.BlockSpec(memory_space=pltpu.VMEM)
    return pl.pallas_call(
        kernel,
        out_shape=outs,
        in_specs=[vmem] * len(args),
        out_specs=[vmem] * len(outs),
        scratch_shapes=scratch,
        compiler_params=pltpu.CompilerParams(vmem_limit_bytes=40 * 1024 * 1024),
        cost_estimate=pl.CostEstimate(flops=flops, bytes_accessed=4_000_000, transcendentals=0),
    )(*args)


def summed_everywhere(parts, axis):
    count = lax.axis_size(axis)
    rows, lanes = parts.shape
    cut = parts.reshape(count, rows // count, lanes)
    arrived = lax.all_to_all(cut, axis, split_axis=0, concat_axis=0, tiled=True)
    own = arrived.astype(jnp.float32).sum(axis=0).astype(jnp.bfloat16)
    copies = jnp.broadcast_to(own, cut.shape)
    return lax.all_to_all(copies, axis, split_axis=0, concat_axis=0, tiled=True).reshape(
        rows, lanes
    )


def on_device(field, x_weight, y_weight, up_weight, up_bias, down_weight):
    _, chans, nx, ny = field.shape
    half = chans // 2
    hid = up_weight.shape[1]
    total_x = nx * lax.axis_size("row")
    total_y = ny * lax.axis_size("col")
    fwd_x, inv_x = table_pair(total_x, lax.axis_index("row") * nx, nx)
    fwd_y, inv_y = table_pair(total_y, lax.axis_index("col") * ny, ny)
    group = 4
    fbx = jnp.kron(jnp.eye(group, dtype=jnp.bfloat16), fwd_x)
    inv_xt = inv_x.T
    mixers = [(mixing_matrices(x_weight[a]), mixing_matrices(y_weight[a])) for a in range(LAYERS)]
    f32, bf16 = jnp.float32, jnp.bfloat16
    parts = [
        jax.ShapeDtypeStruct((chans * ROWS, ny), bf16),
        jax.ShapeDtypeStruct((half * ROWS, 2 * nx), bf16),
    ]
    whole = jax.ShapeDtypeStruct((chans, nx, ny), bf16)
    work = [
        pltpu.VMEM((ROWS * (chans + 8), ny), f32),
        pltpu.VMEM((ROWS * (half + 8), 2 * nx), f32),
        pltpu.VMEM((ROWS * chans, ny), f32),
        pltpu.VMEM((ROWS * half, 2 * nx), f32),
    ]
    tmp = pltpu.VMEM((chans * (nx + 8), ny), f32)
    state = field.reshape(chans, nx, ny)
    mx, my = call(first_kernel, parts, work, [state, fbx, fwd_y, *mixers[0]], 200_000_000)
    for layer in range(LAYERS):
        got_x = summed_everywhere(mx, "row").reshape(chans, ROWS, ny)
        got_y = summed_everywhere(my, "col").reshape(half, ROWS, 2 * nx)
        bias = jnp.broadcast_to(up_bias[layer][:, None], (hid, 4 * ny))
        down = down_weight[layer] * jnp.asarray(0.5, bf16)
        args = [state, got_x, got_y, inv_xt, inv_y, up_weight[layer], bias, down]
        if layer + 1 < LAYERS:
            args += [fbx, fwd_y, *mixers[layer + 1]]
            state, mx, my = call(middle_kernel, [whole, *parts], [tmp, *work], args, 900_000_000)
        else:
            (state,) = call(last_kernel, [whole], [tmp], args, 700_000_000)
    return state.reshape(field.shape)


def solution(mesh):
    in_specs = (P(None, None, "row", "col"), P(), P(), P(), P(), P())
    out_specs = P(None, None, "row", "col")
    return jax.shard_map(
        on_device, mesh=mesh, in_specs=in_specs, out_specs=out_specs, check_vma=False
    )
```

```python
import functools
import math

import jax
import jax.numpy as jnp
from jax import lax
from jax.experimental import pallas as pl
from jax.experimental.pallas import tpu as pltpu
from jax.sharding import PartitionSpec as P


MODES = 12
ROWS = 2 * MODES
LAYERS = 2
ROOT_HALF = math.sqrt(0.5)
NN = (((1,), (0,)), ((), ()))
TN = (((0,), (0,)), ((), ()))
NT = (((1,), (1,)), ((), ()))
F32, BF16 = jnp.float32, jnp.bfloat16
BLOCK = 4
WIDE = 4
AHEAD = 2
PAD = 8
EXTRA = 16


def dot(a, b, dims=NN):
    return lax.dot_general(a, b, dims, preferred_element_type=F32)


def angles(total, start, count):
    pos = start + jnp.arange(count, dtype=jnp.int32)
    kays = jnp.arange(MODES, dtype=jnp.int32)
    phase = kays[:, None] * pos[None, :] % total
    angle = phase.astype(F32) * (2.0 * math.pi / total)
    wave = jnp.concatenate([jnp.cos(angle), -jnp.sin(angle)], axis=0)
    once = jnp.concatenate([kays, kays]) == 0
    factor = (jnp.where(once, 1.0, 2.0) / total).astype(F32)[:, None]
    return wave.astype(BF16), (wave * factor).astype(BF16)


def tables(nx, ny):
    fwd_x, inv_x = angles(nx * lax.axis_size("row"), lax.axis_index("row") * nx, nx)
    fwd_y, inv_y = angles(ny * lax.axis_size("col"), lax.axis_index("col") * ny, ny)
    return jnp.concatenate([fwd_y, inv_y, jnp.concatenate([fwd_x, inv_x], axis=1)], axis=0)


def put(ref, start, size, stride, value):
    ref[pl.ds(start, size, stride=stride), :] = value


def mixer(weight, k):
    real, imag = weight[0, k], weight[1, k]
    top = jnp.concatenate([real, imag], axis=1)
    bottom = jnp.concatenate([-imag, real], axis=1)
    return jnp.concatenate([top, bottom], axis=0).astype(BF16)


def forward_x(state, tab, got, weight, out, work, laid):
    chans, nx, ny = state.shape
    step = work.shape[0] // ROWS
    fwd = tab[2 * ROWS : 3 * ROWS, :nx].astype(F32)
    zero = jnp.zeros_like(fwd)
    lines = []
    for i in range(BLOCK):
        lines.append(jnp.concatenate([fwd if a == i else zero for a in range(BLOCK)], axis=1))
    table = jnp.concatenate(lines, axis=0).astype(BF16)
    for c0 in range(0, chans, BLOCK):
        part = dot(table, state[c0 : c0 + BLOCK].reshape(BLOCK * nx, ny))
        for i in range(BLOCK):
            put(work, c0 + i, ROWS, step, part[i * ROWS : (i + 1) * ROWS])
    got.wait()
    for k in range(MODES):
        re = work[k * step : k * step + chans]
        im = work[(MODES + k) * step : (MODES + k) * step + chans]
        mixed = dot(mixer(weight, k), jnp.concatenate([re, im], axis=0).astype(BF16), TN)
        put(laid, k, chans, ROWS, mixed[:chans])
        put(laid, MODES + k, chans, ROWS, mixed[chans:])
    out[...] = laid[...].astype(BF16)


def forward_y(state, tab, got, weight, out, work, laid):
    chans, nx, _ = state.shape
    half = chans // 2
    step = work.shape[0] // ROWS
    table = tab[:ROWS]
    for j in range(0, half, 2):
        both = [state[j], state[j + half], state[j + 1], state[j + 1 + half]]
        part = dot(table, jnp.concatenate(both, axis=0), NT)
        put(work, j, ROWS, step, part[:, : 2 * nx])
        put(work, j + 1, ROWS, step, part[:, 2 * nx :])
    got.wait()
    for k in range(MODES):
        re = work[k * step : k * step + half]
        im = work[(MODES + k) * step : (MODES + k) * step + half]
        stack = jnp.concatenate([re[:, :nx], re[:, nx:], im[:, :nx], im[:, nx:]], axis=0)
        mixed = dot(mixer(weight, k), stack.astype(BF16), TN)
        re = jnp.concatenate([mixed[:half], mixed[half:chans]], axis=1)
        im = jnp.concatenate([mixed[chans : chans + half], mixed[chans + half :]], axis=1)
        put(laid, k, half, ROWS, re)
        put(laid, MODES + k, half, ROWS, im)
    out[...] = laid[...].astype(BF16)


def add_branches(field, got_x, got_y, tab, tmp):
    chans, nx, _ = field.shape
    half = chans // 2
    step = tmp.shape[0] // chans
    to_y = tab[ROWS : 2 * ROWS]
    to_x = tab[2 * ROWS : 3 * ROWS, nx : 2 * nx].astype(F32).T.astype(BF16)
    for j in range(half):
        from_y = dot(got_y[j], to_y, TN)
        for h in range(2):
            c = j + h * half
            back = dot(to_x, got_x[c]) + from_y[h * nx : (h + 1) * nx]
            total = (field[c].astype(F32) + back).astype(BF16)
            tmp[c * step : c * step + nx] = total.astype(F32)


def feed_forward(layer, up, bias, down, tmp, lifted, nx):
    _, depth, hid = up.shape
    ny = tmp.shape[1]
    step = tmp.shape[0] // depth
    rest = bias[layer : layer + 1, :]
    rows = [up[layer].astype(F32)]
    for _ in range(3):
        part = rest.astype(BF16).astype(F32)
        rows.append(part)
        rest = rest - part
    rows.append(jnp.zeros((EXTRA - 3, hid), F32))
    lifted[...] = jnp.concatenate(rows, axis=0).T.astype(BF16)
    ones = (lax.broadcasted_iota(jnp.int32, (EXTRA, WIDE * ny), 0) < 3).astype(F32).astype(BF16)

    def feed(i, carry):
        x0 = i * (WIDE * AHEAD)
        wides, news = [], []
        for b in range(AHEAD):
            lines = [tmp[pl.ds(x0 + b * WIDE + a, depth, stride=step), :] for a in range(WIDE)]
            wides.append(jnp.concatenate(lines, axis=1))
        for wide in wides:
            hidden = dot(lifted[...], jnp.concatenate([wide.astype(BF16), ones], axis=0))
            hidden = hidden + hidden * lax.erf(hidden * ROOT_HALF)
            back = dot(down[layer] * jnp.asarray(0.5, BF16), hidden.astype(BF16))
            news.append((wide + back).astype(BF16).astype(F32))
        for b in range(AHEAD):
            for a in range(WIDE):
                line = news[b][:, a * ny : (a + 1) * ny]
                put(tmp, x0 + b * WIDE + a, depth, step, line)
        return carry

    lax.fori_loop(0, nx // (WIDE * AHEAD), feed, 0)


def fetch(source, target, sem):
    return pltpu.make_async_copy(source, target, sem)


def first_kernel(field, tab, all_x, all_y, out_x, out_y, qx, qy, rx, ry, wx, wy, sem_x, sem_y):
    get_y = fetch(all_y.at[0], wy, sem_y)
    get_x = fetch(all_x.at[0], wx, sem_x)
    get_y.start()
    get_x.start()
    forward_y(field, tab, get_y, wy, out_y, qy, ry)
    forward_x(field, tab, get_x, wx, out_x, qx, rx)


def layer_kernel(layer, last, field, got_x, got_y, tab, up, bias, down, *refs):
    if last:
        result, tmp, lifted = refs
    else:
        all_x, all_y, result, out_x, out_y, tmp, lifted, qx, qy, rx, ry, wx, wy, sem_x, sem_y = refs
        get_y = fetch(all_y.at[layer + 1], wy, sem_y)
        get_x = fetch(all_x.at[layer + 1], wx, sem_x)
        get_y.start()
        get_x.start()
    chans, nx, _ = field.shape
    step = tmp.shape[0] // chans
    add_branches(field, got_x, got_y, tab, tmp)
    feed_forward(layer, up, bias, down, tmp, lifted, nx)
    for c in range(chans):
        result[c] = tmp[c * step : c * step + nx].astype(BF16)
    if not last:
        forward_y(result, tab, get_y, wy, out_y, qy, ry)
        forward_x(result, tab, get_x, wx, out_x, qx, rx)


def call(kernel, outs, scratch, args, flops, far=0):
    vmem = pl.BlockSpec(memory_space=pltpu.VMEM)
    away = pl.BlockSpec(memory_space=pl.ANY)
    return pl.pallas_call(
        kernel,
        out_shape=outs,
        in_specs=[vmem] * (len(args) - far) + [away] * far,
        out_specs=[vmem] * len(outs),
        scratch_shapes=scratch,
        compiler_params=pltpu.CompilerParams(vmem_limit_bytes=24 * 1024 * 1024),
        cost_estimate=pl.CostEstimate(flops=flops, bytes_accessed=4_000_000, transcendentals=0),
    )(*args)


def exchange(cut, axis):
    return lax.all_to_all(cut, axis, split_axis=0, concat_axis=0, tiled=True)


def chunks(parts, axis):
    count = lax.axis_size(axis)
    return parts.reshape(count, parts.shape[0] // count, parts.shape[1])


def total_of(arrived):
    return arrived.astype(F32).sum(axis=0).astype(BF16)


def summed_everywhere(parts_x, parts_y):
    own_y = total_of(exchange(chunks(parts_y, "col"), "col"))
    arrived = exchange(chunks(parts_x, "row"), "row")
    got_y = lax.all_gather(own_y, "col", axis=0, tiled=True)
    copies = jnp.broadcast_to(total_of(arrived), arrived.shape)
    got_x = exchange(copies, "row")
    return got_x.reshape(parts_x.shape), got_y


def on_device(field, x_weight, y_weight, up_weight, up_bias, down_weight):
    _, chans, nx, ny = field.shape
    half = chans // 2
    hid = up_weight.shape[1]
    tab = tables(nx, ny)
    lifts = jnp.swapaxes(up_weight, 1, 2)
    parts = [
        jax.ShapeDtypeStruct((chans * ROWS, ny), BF16),
        jax.ShapeDtypeStruct((half * ROWS, 2 * nx), BF16),
    ]
    whole = jax.ShapeDtypeStruct((chans, nx, ny), BF16)
    work = [
        pltpu.VMEM((ROWS * (chans + PAD), ny), F32),
        pltpu.VMEM((ROWS * (half + PAD), 2 * nx), F32),
        pltpu.VMEM((ROWS * chans, ny), F32),
        pltpu.VMEM((ROWS * half, 2 * nx), F32),
        pltpu.VMEM(x_weight.shape[1:], F32),
        pltpu.VMEM(y_weight.shape[1:], F32),
        pltpu.SemaphoreType.DMA,
        pltpu.SemaphoreType.DMA,
    ]
    space = [pltpu.VMEM((chans * (nx + PAD), ny), F32), pltpu.VMEM((hid, chans + EXTRA), BF16)]
    state = field.reshape(chans, nx, ny)
    first = [state, tab, x_weight, y_weight]
    mx, my = call(first_kernel, parts, work, first, 200_000_000, 2)
    for layer in range(LAYERS):
        last = layer + 1 == LAYERS
        got_x, got_y = summed_everywhere(mx, my)
        got_x = got_x.reshape(chans, ROWS, ny)
        got_y = got_y.reshape(half, ROWS, 2 * nx)
        args = [state, got_x, got_y, tab, lifts, up_bias, down_weight]
        kernel = functools.partial(layer_kernel, layer, last)
        if last:
            (state,) = call(kernel, [whole], space, args, 700_000_000)
        else:
            args += [x_weight, y_weight]
            state, mx, my = call(kernel, [whole, *parts], [*space, *work], args, 900_000_000, 2)
    return state.reshape(field.shape)


def solution(mesh):
    in_specs = (P(None, None, "row", "col"), P(), P(), P(), P(), P())
    out_specs = P(None, None, "row", "col")
    return jax.shard_map(
        on_device, mesh=mesh, in_specs=in_specs, out_specs=out_specs, check_vma=False
    )
```

```python
import functools
import math

import jax
import jax.numpy as jnp
from jax import lax
from jax.experimental import pallas as pl
from jax.experimental.pallas import tpu as pltpu
from jax.sharding import PartitionSpec as P


MODES = 12
ROWS = 2 * MODES
LAYERS = 2
ROOT_HALF = math.sqrt(0.5)
NN = (((1,), (0,)), ((), ()))
TN = (((0,), (0,)), ((), ()))
NT = (((1,), (1,)), ((), ()))
F32, BF16 = jnp.float32, jnp.bfloat16
BLOCK = 4
WIDE = 16
AHEAD = 2
PAD = 8
EXTRA = 16


def dot(a, b, dims=NN):
    return lax.dot_general(a, b, dims, preferred_element_type=F32)


def angles(total, start, count):
    pos = start + jnp.arange(count, dtype=jnp.int32)
    kays = jnp.arange(MODES, dtype=jnp.int32)
    phase = kays[:, None] * pos[None, :] % total
    angle = phase.astype(F32) * (2.0 * math.pi / total)
    wave = jnp.concatenate([jnp.cos(angle), -jnp.sin(angle)], axis=0)
    once = jnp.concatenate([kays, kays]) == 0
    factor = (jnp.where(once, 1.0, 2.0) / total).astype(F32)[:, None]
    return wave.astype(BF16), (wave * factor).astype(BF16)


def tables(nx, ny):
    fwd_x, inv_x = angles(nx * lax.axis_size("row"), lax.axis_index("row") * nx, nx)
    fwd_y, inv_y = angles(ny * lax.axis_size("col"), lax.axis_index("col") * ny, ny)
    return jnp.concatenate([fwd_y, inv_y, jnp.concatenate([fwd_x, inv_x], axis=1)], axis=0)


def put(ref, start, size, stride, value):
    ref[pl.ds(start, size, stride=stride), :] = value


def mixer(weight, k):
    real, imag = weight[0, k], weight[1, k]
    top = jnp.concatenate([real, imag], axis=1)
    bottom = jnp.concatenate([-imag, real], axis=1)
    return jnp.concatenate([top, bottom], axis=0).astype(BF16)


def forward_x(state, tab, weight, out, work, laid):
    chans, nx, ny = state.shape
    step = work.shape[0] // ROWS
    fwd = tab[2 * ROWS : 3 * ROWS, :nx].astype(F32)
    zero = jnp.zeros_like(fwd)
    lines = []
    for i in range(BLOCK):
        lines.append(jnp.concatenate([fwd if a == i else zero for a in range(BLOCK)], axis=1))
    table = jnp.concatenate(lines, axis=0).astype(BF16)
    for c0 in range(0, chans, BLOCK):
        part = dot(table, state[c0 : c0 + BLOCK].reshape(BLOCK * nx, ny))
        for i in range(BLOCK):
            put(work, c0 + i, ROWS, step, part[i * ROWS : (i + 1) * ROWS])
    for k in range(MODES):
        re = work[k * step : k * step + chans]
        im = work[(MODES + k) * step : (MODES + k) * step + chans]
        mixed = dot(mixer(weight, k), jnp.concatenate([re, im], axis=0).astype(BF16), TN)
        put(laid, k, chans, ROWS, mixed[:chans])
        put(laid, MODES + k, chans, ROWS, mixed[chans:])
    out[...] = laid[...].astype(BF16)


def sums_y(state, tab, work):
    chans, nx, _ = state.shape
    half = chans // 2
    step = work.shape[0] // ROWS
    table = tab[:ROWS]
    for j in range(0, half, 2):
        both = [state[j], state[j + half], state[j + 1], state[j + 1 + half]]
        part = dot(table, jnp.concatenate(both, axis=0), NT)
        put(work, j, ROWS, step, part[:, : 2 * nx])
        put(work, j + 1, ROWS, step, part[:, 2 * nx :])


def mix_y(work, weight, out, laid):
    half, nx = work.shape[0] // ROWS - PAD, work.shape[1] // 2
    chans = 2 * half
    step = work.shape[0] // ROWS
    for k in range(MODES):
        re = work[k * step : k * step + half]
        im = work[(MODES + k) * step : (MODES + k) * step + half]
        stack = jnp.concatenate([re[:, :nx], re[:, nx:], im[:, :nx], im[:, nx:]], axis=0)
        mixed = dot(mixer(weight, k), stack.astype(BF16), TN)
        re = jnp.concatenate([mixed[:half], mixed[half:chans]], axis=1)
        im = jnp.concatenate([mixed[chans : chans + half], mixed[chans + half :]], axis=1)
        put(laid, k, half, ROWS, re)
        put(laid, MODES + k, half, ROWS, im)
    out[...] = laid[...].astype(BF16)


def add_branches(field, got_x, got_y, tab, tmp):
    chans, nx, _ = field.shape
    half = chans // 2
    step = tmp.shape[0] // chans
    to_y = tab[ROWS : 2 * ROWS]
    to_x = tab[2 * ROWS : 3 * ROWS, nx : 2 * nx].astype(F32).T.astype(BF16)
    for j in range(half):
        from_y = dot(got_y[j], to_y, TN)
        for h in range(2):
            c = j + h * half
            back = dot(to_x, got_x[c]) + from_y[h * nx : (h + 1) * nx]
            total = (field[c].astype(F32) + back).astype(BF16)
            tmp[c * step : c * step + nx] = total.astype(F32)


def feed_forward(layer, up, bias, down, tmp, lifted, nx, finish):
    _, depth, hid = up.shape
    ny = tmp.shape[1]
    step = tmp.shape[0] // depth
    rest = bias[layer : layer + 1, :]
    rows = [up[layer].astype(F32)]
    for _ in range(3):
        part = rest.astype(BF16).astype(F32)
        rows.append(part)
        rest = rest - part
    rows.append(jnp.zeros((EXTRA - 3, hid), F32))
    lifted[...] = jnp.concatenate(rows, axis=0).T.astype(BF16)
    ones = (lax.broadcasted_iota(jnp.int32, (EXTRA, WIDE * ny), 0) < 3).astype(F32).astype(BF16)

    for x0 in range(0, nx, WIDE * AHEAD):
        wides, news = [], []
        for b in range(AHEAD):
            lines = [tmp[pl.ds(x0 + b * WIDE + a, depth, stride=step), :] for a in range(WIDE)]
            wides.append(jnp.concatenate(lines, axis=1))
        for wide in wides:
            hidden = dot(lifted[...], jnp.concatenate([wide.astype(BF16), ones], axis=0))
            hidden = hidden + hidden * lax.erf(hidden * ROOT_HALF)
            back = dot(down[layer] * jnp.asarray(0.5, BF16), hidden.astype(BF16))
            news.append((wide + back).astype(BF16).astype(F32))
        for b in range(AHEAD):
            for a in range(WIDE):
                line = news[b][:, a * ny : (a + 1) * ny]
                put(tmp, x0 + b * WIDE + a, depth, step, line)
        finish(x0, WIDE * AHEAD)


def fetch(source, target, sem):
    return pltpu.make_async_copy(source, target, sem)


def mix_kernel(work, weights, out, laid):
    mix_y(work, weights.at[0], out, laid)


def x_kernel(layer, state, tab, weights, out, work, laid):
    forward_x(state, tab, weights.at[layer], out, work, laid)


def layer_kernel(layer, last, field, got_x, got_y, tab, up, bias, down, *refs):
    if last:
        result, tmp, lifted, held, sems = refs
    else:
        weights, result, out, tmp, lifted, held, sems, work, laid = refs
    chans, nx, _ = field.shape
    step = tmp.shape[0] // chans
    add_branches(field, got_x, got_y, tab, tmp)
    copies = []

    def finish(x0, count):
        for c in range(chans):
            row = c * step + x0
            held[c, x0 : x0 + count, :] = tmp[row : row + count].astype(BF16)
        lines = pl.ds(x0, count)
        copy = fetch(held.at[:, lines], result.at[:, lines], sems.at[len(copies)])
        copy.start()
        copies.append(copy)

    feed_forward(layer, up, bias, down, tmp, lifted, nx, finish)
    if not last:
        sums_y(held, tab, work)
        mix_y(work, weights.at[layer + 1], out, laid)
    for copy in copies:
        copy.wait()


def sum_kernel(arrived, copies):
    total = arrived[0].astype(F32)
    for i in range(1, arrived.shape[0]):
        total = total + arrived[i].astype(F32)
    total = total.astype(BF16)
    for i in range(arrived.shape[0]):
        copies[i] = total


def call(kernel, outs, scratch, args, flops, sent=()):
    vmem = pl.BlockSpec(memory_space=pltpu.VMEM)
    away = pl.BlockSpec(memory_space=pl.ANY)
    return pl.pallas_call(
        kernel,
        out_shape=outs,
        in_specs=[vmem] * len(args),
        out_specs=[away if i in sent else vmem for i in range(len(outs))],
        scratch_shapes=scratch,
        compiler_params=pltpu.CompilerParams(vmem_limit_bytes=24 * 1024 * 1024),
        cost_estimate=pl.CostEstimate(flops=flops, bytes_accessed=4_000_000, transcendentals=0),
    )(*args)


def exchange(cut, axis):
    return lax.all_to_all(cut, axis, split_axis=0, concat_axis=0, tiled=True)


def chunks(parts, axis):
    count = lax.axis_size(axis)
    return parts.reshape(count, parts.shape[0] // count, parts.shape[1])


def total_of(arrived):
    return arrived.astype(F32).sum(axis=0).astype(BF16)


def summed_everywhere(parts_y, make_x):
    own_y = total_of(exchange(chunks(parts_y, "col"), "col"))
    parts_x = make_x()
    arrived = exchange(chunks(parts_x, "row"), "row")
    got_y = lax.all_gather(own_y, "col", axis=0, tiled=True)
    shape = jax.ShapeDtypeStruct(arrived.shape, BF16)
    (copies,) = call(sum_kernel, [shape], [], [arrived], 1_000_000)
    got_x = exchange(copies, "row")
    return got_x.reshape(parts_x.shape), got_y


def on_device(field, x_weight, y_weight, up_weight, up_bias, down_weight):
    _, chans, nx, ny = field.shape
    half = chans // 2
    hid = up_weight.shape[1]
    tab = tables(nx, ny)
    lifts = jnp.swapaxes(up_weight, 1, 2)
    part_x = pltpu.HBM((chans * ROWS, ny), BF16)
    part_y = pltpu.HBM((half * ROWS, 2 * nx), BF16)
    whole = pltpu.HBM((chans, nx, ny), BF16)
    work_x = [
        pltpu.VMEM((ROWS * (chans + PAD), ny), F32),
        pltpu.VMEM((ROWS * chans, ny), F32),
    ]
    work_y = [
        pltpu.VMEM((ROWS * (half + PAD), 2 * nx), F32),
        pltpu.VMEM((ROWS * half, 2 * nx), F32),
    ]
    space = [pltpu.VMEM((chans * (nx + PAD), ny), F32), pltpu.VMEM((hid, chans + EXTRA), BF16)]
    one = pltpu.SemaphoreType.DMA
    space += [pltpu.VMEM((chans, nx, ny), BF16), one((nx // (WIDE * AHEAD),))]
    state = field.reshape(chans, nx, ny)
    sums = jax.ShapeDtypeStruct(work_y[0].shape, F32)
    (sums,) = call(sums_y, [sums], [], [state, tab], 60_000_000)
    (my,) = call(mix_kernel, [part_y], work_y[1:], [sums, y_weight], 40_000_000)
    for layer in range(LAYERS):
        last = layer + 1 == LAYERS

        def make_x(state=state, layer=layer):
            args = [state, tab, x_weight]
            kernel = functools.partial(x_kernel, layer)
            return call(kernel, [part_x], work_x, args, 100_000_000)[0]

        got_x, got_y = summed_everywhere(my, make_x)
        got_x = got_x.reshape(chans, ROWS, ny)
        got_y = got_y.reshape(half, ROWS, 2 * nx)
        args = [state, got_x, got_y, tab, lifts, up_bias, down_weight]
        kernel = functools.partial(layer_kernel, layer, last)
        if last:
            (state,) = call(kernel, [whole], space, args, 700_000_000, sent=(0,))
        else:
            args.append(y_weight)
            scratch = [*space, *work_y]
            state, my = call(kernel, [whole, part_y], scratch, args, 900_000_000, sent=(0,))
    return state.reshape(field.shape)


def solution(mesh):
    in_specs = (P(None, None, "row", "col"), P(), P(), P(), P(), P())
    out_specs = P(None, None, "row", "col")
    return jax.shard_map(
        on_device, mesh=mesh, in_specs=in_specs, out_specs=out_specs, check_vma=False
    )
```

```python
import functools
import math

import jax
import jax.numpy as jnp
from jax import lax
from jax.experimental import pallas as pl
from jax.experimental.pallas import tpu as pltpu
from jax.sharding import PartitionSpec as P


MODES = 12
ROWS = 2 * MODES
LAYERS = 2
ROOT_HALF = math.sqrt(0.5)
NN = (((1,), (0,)), ((), ()))
TN = (((0,), (0,)), ((), ()))
NT = (((1,), (1,)), ((), ()))
F32, BF16 = jnp.float32, jnp.bfloat16
BLOCK = 4
WIDE = 16
AHEAD = 2
PAD = 8
EXTRA = 16


def dot(a, b, dims=NN):
    return lax.dot_general(a, b, dims, preferred_element_type=F32)


def angles(total, start, count):
    pos = start + jnp.arange(count, dtype=jnp.int32)
    kays = jnp.arange(MODES, dtype=jnp.int32)
    phase = kays[:, None] * pos[None, :] % total
    angle = phase.astype(F32) * (2.0 * math.pi / total)
    wave = jnp.concatenate([jnp.cos(angle), -jnp.sin(angle)], axis=0)
    once = jnp.concatenate([kays, kays]) == 0
    factor = (jnp.where(once, 1.0, 2.0) / total).astype(F32)[:, None]
    return wave.astype(BF16), (wave * factor).astype(BF16)


def tables(nx, ny):
    fwd_x, inv_x = angles(nx * lax.axis_size("row"), lax.axis_index("row") * nx, nx)
    fwd_y, inv_y = angles(ny * lax.axis_size("col"), lax.axis_index("col") * ny, ny)
    return jnp.concatenate([fwd_y, inv_y, jnp.concatenate([fwd_x, inv_x], axis=1)], axis=0)


def put(ref, start, size, stride, value):
    ref[pl.ds(start, size, stride=stride), :] = value


def mixer(weight, k):
    real, imag = weight[0, k], weight[1, k]
    top = jnp.concatenate([real, imag], axis=1)
    bottom = jnp.concatenate([-imag, real], axis=1)
    return jnp.concatenate([top, bottom], axis=0).astype(BF16)


def forward_x(state, tab, mixing, weight, out, work, laid):
    chans, nx, ny = state.shape
    step = work.shape[0] // ROWS
    fwd = tab[2 * ROWS : 3 * ROWS, :nx].astype(F32)
    zero = jnp.zeros_like(fwd)
    lines = []
    for i in range(BLOCK):
        lines.append(jnp.concatenate([fwd if a == i else zero for a in range(BLOCK)], axis=1))
    table = jnp.concatenate(lines, axis=0).astype(BF16)
    for c0 in range(0, chans, BLOCK):
        part = dot(table, state[c0 : c0 + BLOCK].reshape(BLOCK * nx, ny))
        for i in range(BLOCK):
            put(work, c0 + i, ROWS, step, part[i * ROWS : (i + 1) * ROWS])
    mixing.wait()
    for k in range(MODES):
        re = work[k * step : k * step + chans]
        im = work[(MODES + k) * step : (MODES + k) * step + chans]
        mixed = dot(mixer(weight, k), jnp.concatenate([re, im], axis=0).astype(BF16), TN)
        put(laid, k, chans, ROWS, mixed[:chans])
        put(laid, MODES + k, chans, ROWS, mixed[chans:])
    out[...] = laid[...].astype(BF16)


def sums_y(state, tab, out, work):
    chans, nx, _ = state.shape
    half = chans // 2
    step = work.shape[0] // ROWS
    table = tab[:ROWS]
    for j in range(0, half, 2):
        both = [state[j], state[j + half], state[j + 1], state[j + 1 + half]]
        part = dot(table, jnp.concatenate(both, axis=0), NT)
        put(work, j, ROWS, step, part[:, : 2 * nx])
        put(work, j + 1, ROWS, step, part[:, 2 * nx :])
    for m in range(ROWS):
        out[m * half : (m + 1) * half] = work[m * step : m * step + half].astype(BF16)


def y_kernel(layer, got, weights, out, laid, weight, sem):
    mixing = fetch(weights.at[layer], weight, sem)
    mixing.start()
    half, nx = got.shape[0] // ROWS, got.shape[1] // 2
    chans = 2 * half
    mixing.wait()
    for k in range(MODES):
        re = got[k * half : (k + 1) * half]
        im = got[(MODES + k) * half : (MODES + k + 1) * half]
        stack = jnp.concatenate([re[:, :nx], re[:, nx:], im[:, :nx], im[:, nx:]], axis=0)
        mixed = dot(mixer(weight, k), stack, TN)
        re = jnp.concatenate([mixed[:half], mixed[half:chans]], axis=1)
        im = jnp.concatenate([mixed[chans : chans + half], mixed[chans + half :]], axis=1)
        put(laid, k, half, ROWS, re)
        put(laid, MODES + k, half, ROWS, im)
    out[...] = laid[...].astype(BF16)


def add_branches(field, got_x, got_y, tab, tmp):
    chans, nx, _ = field.shape
    half = chans // 2
    step = tmp.shape[0] // chans
    to_y = tab[ROWS : 2 * ROWS]
    to_x = tab[2 * ROWS : 3 * ROWS, nx : 2 * nx].astype(F32).T.astype(BF16)
    for j in range(half):
        from_y = dot(got_y[j], to_y, TN)
        for h in range(2):
            c = j + h * half
            back = dot(to_x, got_x[c]) + from_y[h * nx : (h + 1) * nx]
            total = (field[c].astype(F32) + back).astype(BF16)
            tmp[c * step : c * step + nx] = total.astype(F32)


def feed_forward(layer, up, bias, down, tmp, lifted, nx, finish):
    _, depth, hid = up.shape
    ny = tmp.shape[1]
    step = tmp.shape[0] // depth
    rest = bias[layer : layer + 1, :]
    rows = [up[layer].astype(F32)]
    for _ in range(3):
        part = rest.astype(BF16).astype(F32)
        rows.append(part)
        rest = rest - part
    rows.append(jnp.zeros((EXTRA - 3, hid), F32))
    lifted[...] = jnp.concatenate(rows, axis=0).T.astype(BF16)
    ones = (lax.broadcasted_iota(jnp.int32, (EXTRA, WIDE * ny), 0) < 3).astype(F32).astype(BF16)

    for x0 in range(0, nx, WIDE * AHEAD):
        wides, news = [], []
        for b in range(AHEAD):
            lines = [tmp[pl.ds(x0 + b * WIDE + a, depth, stride=step), :] for a in range(WIDE)]
            wides.append(jnp.concatenate(lines, axis=1))
        for wide in wides:
            hidden = dot(lifted[...], jnp.concatenate([wide.astype(BF16), ones], axis=0))
            hidden = hidden + hidden * lax.erf(hidden * ROOT_HALF)
            back = dot(down[layer] * jnp.asarray(0.5, BF16), hidden.astype(BF16))
            news.append((wide + back).astype(BF16).astype(F32))
        for b in range(AHEAD):
            for a in range(WIDE):
                line = news[b][:, a * ny : (a + 1) * ny]
                put(tmp, x0 + b * WIDE + a, depth, step, line)
        finish(x0, WIDE * AHEAD)


def fetch(source, target, sem):
    return pltpu.make_async_copy(source, target, sem)


def x_kernel(layer, state, tab, weights, out, work, laid, weight, sem):
    mixing = fetch(weights.at[layer], weight, sem)
    mixing.start()
    forward_x(state, tab, mixing, weight, out, work, laid)


def layer_kernel(layer, last, field, got_x, got_y, tab, up, bias, down, *refs):
    if last:
        result, tmp, lifted, held, sems = refs
    else:
        result, out, tmp, lifted, held, sems, work = refs
    chans, nx, _ = field.shape
    step = tmp.shape[0] // chans
    add_branches(field, got_x, got_y, tab, tmp)
    copies = []

    def finish(x0, count):
        for c in range(chans):
            row = c * step + x0
            held[c, x0 : x0 + count, :] = tmp[row : row + count].astype(BF16)
        lines = pl.ds(x0, count)
        copy = fetch(held.at[:, lines], result.at[:, lines], sems.at[len(copies)])
        copy.start()
        copies.append(copy)

    feed_forward(layer, up, bias, down, tmp, lifted, nx, finish)
    if not last:
        sums_y(held, tab, out, work)
    for copy in copies:
        copy.wait()


def summed(arrived):
    total = arrived[0].astype(F32)
    for i in range(1, arrived.shape[0]):
        total = total + arrived[i].astype(F32)
    return total.astype(BF16)


def sum_kernel(arrived, out):
    out[...] = summed(arrived)


def copies_kernel(arrived, copies):
    total = summed(arrived)
    for i in range(arrived.shape[0]):
        copies[i] = total


def call(kernel, outs, scratch, args, flops, sent=(), far=0):
    vmem = pl.BlockSpec(memory_space=pltpu.VMEM)
    away = pl.BlockSpec(memory_space=pl.ANY)
    return pl.pallas_call(
        kernel,
        out_shape=outs,
        in_specs=[vmem] * (len(args) - far) + [away] * far,
        out_specs=[away if i in sent else vmem for i in range(len(outs))],
        scratch_shapes=scratch,
        compiler_params=pltpu.CompilerParams(vmem_limit_bytes=24 * 1024 * 1024),
        cost_estimate=pl.CostEstimate(flops=flops, bytes_accessed=4_000_000, transcendentals=0),
    )(*args)


def exchange(cut, axis):
    return lax.all_to_all(cut, axis, split_axis=0, concat_axis=0, tiled=True)


def chunks(parts, axis):
    count = lax.axis_size(axis)
    return parts.reshape(count, parts.shape[0] // count, parts.shape[1])


def on_device(field, x_weight, y_weight, up_weight, up_bias, down_weight):
    _, chans, nx, ny = field.shape
    half = chans // 2
    hid = up_weight.shape[1]
    tab = tables(nx, ny)
    lifts = jnp.swapaxes(up_weight, 1, 2)
    part_x = pltpu.HBM((chans * ROWS, ny), BF16)
    part_y = pltpu.HBM((half * ROWS, 2 * nx), BF16)
    whole = pltpu.HBM((chans, nx, ny), BF16)
    wide = jax.ShapeDtypeStruct((half * ROWS, 2 * nx), BF16)
    weight = [pltpu.VMEM(x_weight.shape[1:], F32), pltpu.SemaphoreType.DMA]
    x_far = pltpu.with_memory_space_constraint(x_weight, pltpu.HBM)
    y_far = pltpu.with_memory_space_constraint(y_weight, pltpu.HBM)
    work_x = [pltpu.VMEM((ROWS * (chans + PAD), ny), F32), pltpu.VMEM((ROWS * chans, ny), F32)]
    work_x += weight
    work_y = [pltpu.VMEM((ROWS * (half + PAD), 2 * nx), F32)]
    laid_y = [pltpu.VMEM((ROWS * half, 2 * nx), F32), *weight]
    space = [
        pltpu.VMEM((chans * (nx + PAD), ny), F32),
        pltpu.VMEM((hid, chans + EXTRA), BF16),
        pltpu.VMEM((chans, nx, ny), BF16),
        pltpu.SemaphoreType.DMA((nx // (WIDE * AHEAD),)),
    ]
    state = field.reshape(chans, nx, ny)
    (parts_y,) = call(sums_y, [part_y], work_y, [state, tab], 60_000_000)
    for layer in range(LAYERS):
        last = layer + 1 == LAYERS
        arrived = exchange(chunks(parts_y, "col"), "col")
        shape = jax.ShapeDtypeStruct(arrived.shape[1:], BF16)
        (own_y,) = call(sum_kernel, [shape], [], [arrived], 1_000_000)
        kernel = functools.partial(x_kernel, layer)
        (parts_x,) = call(kernel, [part_x], work_x, [state, tab, x_far], 100_000_000, far=1)
        arrived = exchange(chunks(parts_x, "row"), "row")
        shape = pltpu.HBM(arrived.shape, BF16)
        (copies,) = call(copies_kernel, [shape], [], [arrived], 1_000_000)
        got_x = exchange(copies, "row").reshape(chans, ROWS, ny)
        got_y = lax.all_gather(own_y, "col", axis=0, tiled=True)
        kernel = functools.partial(y_kernel, layer)
        (mixed_y,) = call(kernel, [wide], laid_y, [got_y, y_far], 40_000_000, far=1)
        mixed_y = mixed_y.reshape(half, ROWS, 2 * nx)
        args = [state, got_x, mixed_y, tab, lifts, up_bias, down_weight]
        kernel = functools.partial(layer_kernel, layer, last)
        if last:
            (state,) = call(kernel, [whole], space, args, 700_000_000, sent=(0,))
        else:
            scratch = [*space, *work_y]
            state, parts_y = call(kernel, [whole, part_y], scratch, args, 900_000_000, sent=(0,))
    return state.reshape(field.shape)


def solution(mesh):
    in_specs = (P(None, None, "row", "col"), P(), P(), P(), P(), P())
    out_specs = P(None, None, "row", "col")
    return jax.shard_map(
        on_device, mesh=mesh, in_specs=in_specs, out_specs=out_specs, check_vma=False
    )
```

```python
import functools
import math

import jax
import jax.numpy as jnp
from jax import lax
from jax.experimental import pallas as pl
from jax.experimental.pallas import tpu as pltpu
from jax.sharding import PartitionSpec as P


MODES = 12
ROWS = 2 * MODES
LAYERS = 2
ROOT_HALF = math.sqrt(0.5)
NN = (((1,), (0,)), ((), ()))
TN = (((0,), (0,)), ((), ()))
NT = (((1,), (1,)), ((), ()))
F32, BF16 = jnp.float32, jnp.bfloat16
BLOCK = 4
WIDE = 16
AHEAD = 2
PAD = 8
EXTRA = 16


def dot(a, b, dims=NN):
    return lax.dot_general(a, b, dims, preferred_element_type=F32)


def angles(total, start, count):
    pos = start + jnp.arange(count, dtype=jnp.int32)
    kays = jnp.arange(MODES, dtype=jnp.int32)
    phase = kays[:, None] * pos[None, :] % total
    angle = phase.astype(F32) * (2.0 * math.pi / total)
    wave = jnp.concatenate([jnp.cos(angle), -jnp.sin(angle)], axis=0)
    once = jnp.concatenate([kays, kays]) == 0
    factor = (jnp.where(once, 1.0, 2.0) / total).astype(F32)[:, None]
    return wave.astype(BF16), (wave * factor).astype(BF16)


def tables(nx, ny):
    fwd_x, inv_x = angles(nx * lax.axis_size("row"), lax.axis_index("row") * nx, nx)
    fwd_y, inv_y = angles(ny * lax.axis_size("col"), lax.axis_index("col") * ny, ny)
    return jnp.concatenate([fwd_y, inv_y, jnp.concatenate([fwd_x, inv_x], axis=1)], axis=0)


def put(ref, start, size, stride, value):
    ref[pl.ds(start, size, stride=stride), :] = value


def mixer(weight, k):
    real, imag = weight[0, k], weight[1, k]
    top = jnp.concatenate([real, imag], axis=1)
    bottom = jnp.concatenate([-imag, real], axis=1)
    return jnp.concatenate([top, bottom], axis=0)


def forward_x(state, tab, mixing, weight, out, work, laid):
    chans, nx, ny = state.shape
    step = work.shape[0] // ROWS
    fwd = tab[2 * ROWS : 3 * ROWS, :nx].astype(F32)
    zero = jnp.zeros_like(fwd)
    lines = []
    for i in range(BLOCK):
        lines.append(jnp.concatenate([fwd if a == i else zero for a in range(BLOCK)], axis=1))
    table = jnp.concatenate(lines, axis=0).astype(BF16)
    for c0 in range(0, chans, BLOCK):
        part = dot(table, state[c0 : c0 + BLOCK].reshape(BLOCK * nx, ny))
        for i in range(BLOCK):
            put(work, c0 + i, ROWS, step, part[i * ROWS : (i + 1) * ROWS])
    mixing.wait()
    for k in range(MODES):
        re = work[k * step : k * step + chans]
        im = work[(MODES + k) * step : (MODES + k) * step + chans]
        mixed = dot(mixer(weight, k).astype(BF16), jnp.concatenate([re, im], axis=0).astype(BF16), TN)
        put(laid, k, chans, ROWS, mixed[:chans])
        put(laid, MODES + k, chans, ROWS, mixed[chans:])
    out[...] = laid[...].astype(BF16)


def sums_y(state, tab, out, work):
    chans, nx, _ = state.shape
    half = chans // 2
    step = work.shape[0] // ROWS
    table = tab[:ROWS]
    for j in range(0, half, 2):
        both = [state[j], state[j + half], state[j + 1], state[j + 1 + half]]
        part = dot(table, jnp.concatenate(both, axis=0), NT)
        put(work, j, ROWS, step, part[:, : 2 * nx])
        put(work, j + 1, ROWS, step, part[:, 2 * nx :])
    for m in range(ROWS):
        out[m * half : (m + 1) * half] = work[m * step : m * step + half].astype(BF16)


def y_kernel(got, mixers, out, laid):
    half, nx = got.shape[0] // ROWS, got.shape[1] // 2
    chans = 2 * half
    for k in range(MODES):
        re = got[k * half : (k + 1) * half]
        im = got[(MODES + k) * half : (MODES + k + 1) * half]
        stack = jnp.concatenate([re[:, :nx], re[:, nx:], im[:, :nx], im[:, nx:]], axis=0)
        mixed = dot(mixers[k], stack)
        re = jnp.concatenate([mixed[:half], mixed[half:chans]], axis=1)
        im = jnp.concatenate([mixed[chans : chans + half], mixed[chans + half :]], axis=1)
        put(laid, k, half, ROWS, re)
        put(laid, MODES + k, half, ROWS, im)
    out[...] = laid[...].astype(BF16)


def add_branches(field, got_x, got_y, tab, tmp):
    chans, nx, _ = field.shape
    half = chans // 2
    step = tmp.shape[0] // chans
    to_y = tab[ROWS : 2 * ROWS]
    to_x = tab[2 * ROWS : 3 * ROWS, nx : 2 * nx].astype(F32).T.astype(BF16)
    for j in range(half):
        from_y = dot(got_y[j], to_y, TN)
        for h in range(2):
            c = j + h * half
            back = dot(to_x, got_x[c]) + from_y[h * nx : (h + 1) * nx]
            total = (field[c].astype(F32) + back).astype(BF16)
            tmp[c * step : c * step + nx] = total.astype(F32)


def feed_forward(layer, up, bias, down, tmp, lifted, nx, finish):
    _, depth, hid = up.shape
    ny = tmp.shape[1]
    step = tmp.shape[0] // depth
    rest = bias[layer : layer + 1, :]
    rows = [up[layer].astype(F32)]
    for _ in range(3):
        part = rest.astype(BF16).astype(F32)
        rows.append(part)
        rest = rest - part
    rows.append(jnp.zeros((EXTRA - 3, hid), F32))
    lifted[...] = jnp.concatenate(rows, axis=0).T.astype(BF16)
    ones = (lax.broadcasted_iota(jnp.int32, (EXTRA, WIDE * ny), 0) < 3).astype(F32).astype(BF16)

    for x0 in range(0, nx, WIDE * AHEAD):
        wides, news = [], []
        for b in range(AHEAD):
            lines = [tmp[pl.ds(x0 + b * WIDE + a, depth, stride=step), :] for a in range(WIDE)]
            wides.append(jnp.concatenate(lines, axis=1))
        for wide in wides:
            hidden = dot(lifted[...], jnp.concatenate([wide.astype(BF16), ones], axis=0))
            hidden = hidden + hidden * lax.erf(hidden * ROOT_HALF)
            back = dot(down[layer] * jnp.asarray(0.5, BF16), hidden.astype(BF16))
            news.append((wide + back).astype(BF16).astype(F32))
        for b in range(AHEAD):
            for a in range(WIDE):
                line = news[b][:, a * ny : (a + 1) * ny]
                put(tmp, x0 + b * WIDE + a, depth, step, line)
        finish(x0, WIDE * AHEAD)


def fetch(source, target, sem):
    return pltpu.make_async_copy(source, target, sem)


def x_kernel(layer, state, tab, all_x, all_y, out, mixers, work, laid, weight, other, sems):
    mixing = fetch(all_x.at[layer], weight, sems.at[0])
    mixing.start()
    later = fetch(all_y.at[layer], other, sems.at[1])
    later.start()
    forward_x(state, tab, mixing, weight, out, work, laid)
    later.wait()
    for k in range(MODES):
        mixers[k] = mixer(other, k).T.astype(BF16)


def layer_kernel(layer, last, field, got_x, got_y, tab, up, bias, down, *refs):
    if last:
        result, tmp, lifted, held, sems = refs
    else:
        result, out, tmp, lifted, held, sems, work = refs
    chans, nx, _ = field.shape
    step = tmp.shape[0] // chans
    add_branches(field, got_x, got_y, tab, tmp)
    copies = []

    def finish(x0, count):
        for c in range(chans):
            row = c * step + x0
            held[c, x0 : x0 + count, :] = tmp[row : row + count].astype(BF16)
        lines = pl.ds(x0, count)
        copy = fetch(held.at[:, lines], result.at[:, lines], sems.at[len(copies)])
        copy.start()
        copies.append(copy)

    feed_forward(layer, up, bias, down, tmp, lifted, nx, finish)
    if not last:
        sums_y(held, tab, out, work)
    for copy in copies:
        copy.wait()


def summed(arrived):
    total = arrived[0].astype(F32)
    for i in range(1, arrived.shape[0]):
        total = total + arrived[i].astype(F32)
    return total.astype(BF16)


def sum_kernel(arrived, out):
    out[...] = summed(arrived)


def copies_kernel(arrived, copies):
    total = summed(arrived)
    for i in range(arrived.shape[0]):
        copies[i] = total


def call(kernel, outs, scratch, args, flops, sent=(), far=0):
    vmem = pl.BlockSpec(memory_space=pltpu.VMEM)
    away = pl.BlockSpec(memory_space=pl.ANY)
    return pl.pallas_call(
        kernel,
        out_shape=outs,
        in_specs=[vmem] * (len(args) - far) + [away] * far,
        out_specs=[away if i in sent else vmem for i in range(len(outs))],
        scratch_shapes=scratch,
        compiler_params=pltpu.CompilerParams(vmem_limit_bytes=24 * 1024 * 1024),
        cost_estimate=pl.CostEstimate(flops=flops, bytes_accessed=4_000_000, transcendentals=0),
    )(*args)


def exchange(cut, axis):
    return lax.all_to_all(cut, axis, split_axis=0, concat_axis=0, tiled=True)


def chunks(parts, axis):
    count = lax.axis_size(axis)
    return parts.reshape(count, parts.shape[0] // count, parts.shape[1])


def on_device(field, x_weight, y_weight, up_weight, up_bias, down_weight):
    _, chans, nx, ny = field.shape
    half = chans // 2
    hid = up_weight.shape[1]
    tab = tables(nx, ny)
    lifts = jnp.swapaxes(up_weight, 1, 2)
    part_x = pltpu.HBM((chans * ROWS, ny), BF16)
    part_y = pltpu.HBM((half * ROWS, 2 * nx), BF16)
    whole = pltpu.HBM((chans, nx, ny), BF16)
    wide = jax.ShapeDtypeStruct((half * ROWS, 2 * nx), BF16)
    mixers = jax.ShapeDtypeStruct((MODES, 2 * chans, 2 * chans), BF16)
    x_far = pltpu.with_memory_space_constraint(x_weight, pltpu.HBM)
    y_far = pltpu.with_memory_space_constraint(y_weight, pltpu.HBM)
    work_x = [pltpu.VMEM((ROWS * (chans + PAD), ny), F32), pltpu.VMEM((ROWS * chans, ny), F32)]
    work_x += [pltpu.VMEM(x_weight.shape[1:], F32), pltpu.VMEM(y_weight.shape[1:], F32)]
    work_x.append(pltpu.SemaphoreType.DMA((2,)))
    work_y = [pltpu.VMEM((ROWS * (half + PAD), 2 * nx), F32)]
    laid_y = [pltpu.VMEM((ROWS * half, 2 * nx), F32)]
    space = [
        pltpu.VMEM((chans * (nx + PAD), ny), F32),
        pltpu.VMEM((hid, chans + EXTRA), BF16),
        pltpu.VMEM((chans, nx, ny), BF16),
        pltpu.SemaphoreType.DMA((nx // (WIDE * AHEAD),)),
    ]
    state = field.reshape(chans, nx, ny)
    (parts_y,) = call(sums_y, [part_y], work_y, [state, tab], 60_000_000)
    for layer in range(LAYERS):
        last = layer + 1 == LAYERS
        arrived = exchange(chunks(parts_y, "col"), "col")
        shape = jax.ShapeDtypeStruct(arrived.shape[1:], BF16)
        (own_y,) = call(sum_kernel, [shape], [], [arrived], 1_000_000)
        kernel = functools.partial(x_kernel, layer)
        args = [state, tab, x_far, y_far]
        parts_x, mix_y = call(kernel, [part_x, mixers], work_x, args, 100_000_000, far=2)
        arrived = exchange(chunks(parts_x, "row"), "row")
        shape = pltpu.HBM(arrived.shape, BF16)
        (copies,) = call(copies_kernel, [shape], [], [arrived], 1_000_000)
        got_x = exchange(copies, "row").reshape(chans, ROWS, ny)
        got_y = lax.all_gather(own_y, "col", axis=0, tiled=True)
        (mixed_y,) = call(y_kernel, [wide], laid_y, [got_y, mix_y], 40_000_000)
        mixed_y = mixed_y.reshape(half, ROWS, 2 * nx)
        args = [state, got_x, mixed_y, tab, lifts, up_bias, down_weight]
        kernel = functools.partial(layer_kernel, layer, last)
        if last:
            (state,) = call(kernel, [whole], space, args, 700_000_000, sent=(0,))
        else:
            scratch = [*space, *work_y]
            state, parts_y = call(kernel, [whole, part_y], scratch, args, 900_000_000, sent=(0,))
    return state.reshape(field.shape)


def solution(mesh):
    in_specs = (P(None, None, "row", "col"), P(), P(), P(), P(), P())
    out_specs = P(None, None, "row", "col")
    return jax.shard_map(
        on_device, mesh=mesh, in_specs=in_specs, out_specs=out_specs, check_vma=False
    )
```
